32 devices in a mesh: obs: 2 (over y), bt: 4 (over z), freq: 2 (over x), pol: 2 (over core).
Axes of the slice: x: 2, y: 2, z: 4, core: 2. Of those that a mesh axis runs over, the one named last changes fastest.
Arguments:
- gains: float32 [16, 4, 8, 1984], P(('obs', 'bt', 'pol'), 'freq'), parts along dimension 0, may hold values from -3 to 3
- visibilities: bfloat16 [16, 4, 8, 4096], P('obs', 'freq', None, ('bt', 'pol')), parts along dimension 0, may hold values from -6 to 6
- first_station: int32 [8192], P(('obs', 'bt', 'pol')), parts along dimension 0, may hold values from 0 to 61
- second_station: int32 [8192], P(('obs', 'bt', 'pol')), parts along dimension 0, may hold values from 0 to 61, as said below
- filled_row_count: int32 [16], P(('obs', 'bt', 'pol')), parts along dimension 0, may hold values from 256 to 512
- facet_dir: int32 [16], P('obs'), parts along dimension 0, may hold values from 0 to 7, each once
Outputs:
- corrected: bfloat16 [16, 4, 8, 4096], P('obs', 'freq', None, ('bt', 'pol')), parts along dimension 0
The draws below stay inside these ranges and needn't reach their ends.
There are 2 independent parts, one for each index of `obs`. The reference program is written for one: setup_inputs(seed, part) draws one part's arguments, and reference() takes and returns one part's arrays. A program takes and returns all parts, laid end to end along the dimension named above; each array names one. Nothing has to cross between parts.
Inputs may be any that keep to these rules, and one draw needn't show every extreme that they name: In every row second_station differs from first_station. `facet_dir`: each direction names exactly one facet.
All inputs are finite; a program needn't handle non-finite values.
Results may differ from the reference program's by a relative error of at most 0.001.
Values sent between devices are 32-bit elements; how exact they have to be, the bound alone decides.
A program may use at most 64 MiB of HBM per device.

```python
import jax
import jax.numpy as jnp
from jax import lax

ARRAY_STATIONS = 62
GAIN_SLOT_COUNT = 4
BLOCK_ROW_COUNT = 512
BLOCKS = 8
DIRS = 8
FACETS = 8
CHANS = 4
TIMES = 32
ROWS = 4096


def station_pair(key):
    folded = jax.random.fold_in(key, 17)
    first_key, second_key = jax.random.split(folded)
    first = jax.random.randint(first_key, (ROWS,), 0, ARRAY_STATIONS, dtype=jnp.int32)
    offset = jax.random.randint(second_key, (ROWS,), 1, ARRAY_STATIONS, dtype=jnp.int32)
    return (first, (first + offset) % ARRAY_STATIONS)


def draw_first_station(key, part):
    return station_pair(key)[0]


def draw_second_station(key, part):
    return station_pair(key)[1]


def with_ends(array, stream_key, low, largest):
    longest = array.shape.index(max(array.shape))
    spots = []
    for shift in (0, 1):
        where = [jax.random.randint(jax.random.fold_in(stream_key, axis), (), 0, length) for axis, length in enumerate(array.shape)]
        where[longest] = (where[longest] + shift) % array.shape[longest]
        spots.append(tuple(where))
    return array.at[spots[0]].set(low).at[spots[1]].set(largest)


def levels(rng, shape, pieces, low, largest):
    def one(dim, shards_of):
        heights = jax.random.uniform(jax.random.fold_in(jax.random.fold_in(rng, 6), dim), (shards_of,), jnp.float32, low / len(pieces), largest / len(pieces))
        return jnp.repeat(jnp.exp(heights), shape[dim] // shards_of).reshape((-1,) + (1,) * (len(shape) - dim - 1))

    level = one(*pieces[0])
    for cut in pieces[1:]:
        level = level * one(*cut)
    return level


def centred(own_key, shape, spread, most, cuts=(), kind=jnp.bfloat16):
    level = levels(own_key, shape, cuts, -0.22, 0.18) if cuts else 1.0
    result = jax.random.normal(own_key, shape, jnp.float32) * spread * level
    return jnp.minimum(jnp.maximum(result, -most), most).astype(kind)


def setup_inputs(seed: int = 0, part: int = 0) -> dict:
    streams_of = jax.random.split(jax.random.key(seed), 7)
    part_keys = jax.random.split(jax.random.fold_in(streams_of[6], part), 7)
    gains = centred(part_keys[0], (DIRS, CHANS, 8, TIMES * ARRAY_STATIONS), 0.5, 3.0, ((0, 8), (1, 2)), jnp.float32)
    visibilities = centred(part_keys[1], (FACETS, CHANS, 8, ROWS), 1.0, 6.0, ((1, 2), (3, 8)))
    first_station = draw_first_station(jax.random.fold_in(jax.random.fold_in(streams_of[6], part), 71), part)
    second_station = draw_second_station(jax.random.fold_in(jax.random.fold_in(streams_of[6], part), 71), part)
    filled_row_count = with_ends(jax.random.randint(part_keys[4], (BLOCKS,), BLOCK_ROW_COUNT // 2, BLOCK_ROW_COUNT + 1), jax.random.fold_in(part_keys[4], 1), BLOCK_ROW_COUNT // 2, BLOCK_ROW_COUNT).astype(jnp.int32)
    facet_dir = jax.random.permutation(part_keys[5], DIRS).astype(jnp.int32)
    return dict(gains=gains, visibilities=visibilities, first_station=first_station, second_station=second_station, filled_row_count=filled_row_count, facet_dir=facet_dir)


def entry(values, row_at, col_at):
    return values[..., 2 * row_at + col_at, :], values[..., 4 + 2 * row_at + col_at, :]


def apply_jones(left_matrix, data, right_matrix):
    real_parts = []
    imag_parts = []
    for out_row in (0, 1):
        for out_col in (0, 1):
            total_re = jnp.zeros_like(left_matrix[..., 0, :])
            total_im = jnp.zeros_like(left_matrix[..., 0, :])
            for middle in (0, 1):
                for column in (0, 1):
                    left_re, left_im = entry(left_matrix, out_row, middle)
                    data_re, data_im = entry(data, middle, column)
                    right_re, right_im = entry(right_matrix, out_col, column)
                    prod_re = left_re * data_re - left_im * data_im
                    prod_im = left_re * data_im + left_im * data_re
                    total_re = total_re + prod_re * right_re + prod_im * right_im
                    total_im = total_im + prod_im * right_re - prod_re * right_im
            real_parts.append(total_re)
            imag_parts.append(total_im)
    return jnp.stack(real_parts + imag_parts, axis=-2)


def slot_blend_weight(antenna, block_rows, slots, stations):
    row_ids = jnp.arange(block_rows, dtype=jnp.int32)
    per_slot = block_rows // slots
    row_slot = row_ids // per_slot
    fraction = ((row_ids % per_slot).astype(jnp.float32) + 0.5) / per_slot
    slot_ids = jnp.arange(slots + 1, dtype=jnp.int32)[:, None, None]
    station_ids = jnp.arange(stations, dtype=jnp.int32)[None, :, None]
    time_weight = jnp.where(slot_ids == row_slot[None, None, :], 1.0 - fraction, 0.0 * fraction)
    time_weight = time_weight + jnp.where(slot_ids == row_slot[None, None, :] + 1, fraction, 0.0 * fraction)
    station_mask = (station_ids == antenna[None, None, :]).astype(jnp.float32)
    weights_table = time_weight * station_mask
    return weights_table.reshape((slots + 1) * stations, block_rows)


def apply_correction(gain_window, block_visibilities, first_station_gain, second_station_gain, filled_rows):
    block_rows = block_visibilities.shape[3]
    left_matrix = jnp.einsum("hsxv,va->hsxa", gain_window, slot_blend_weight(first_station_gain, block_rows, GAIN_SLOT_COUNT, ARRAY_STATIONS), precision=lax.Precision.HIGHEST)
    right_matrix = jnp.einsum("hsxv,va->hsxa", gain_window, slot_blend_weight(second_station_gain, block_rows, GAIN_SLOT_COUNT, ARRAY_STATIONS), precision=lax.Precision.HIGHEST)
    product = apply_jones(left_matrix, block_visibilities.astype(jnp.float32), right_matrix)
    live_mask = jnp.arange(block_rows, dtype=jnp.int32) < filled_rows
    return jnp.where(live_mask, product, 0.0 * product).astype(jnp.bfloat16)


def reference(gains, visibilities, first_station, second_station, filled_row_count, facet_dir):
    onehot = (facet_dir[:, None] == jnp.arange(DIRS, dtype=jnp.int32)[None, :]).astype(jnp.float32)
    chosen = jnp.einsum("fd,dckn->fckn", onehot, gains, precision=lax.Precision.HIGHEST)
    final_slot = chosen[..., (TIMES - 1) * ARRAY_STATIONS:]
    extended = jnp.concatenate([chosen, final_slot], axis=3)

    def one_block(block_index):
        gain_window = lax.dynamic_slice_in_dim(extended, block_index * (GAIN_SLOT_COUNT * ARRAY_STATIONS), (GAIN_SLOT_COUNT + 1) * ARRAY_STATIONS, 3)
        block_visibilities = lax.dynamic_slice_in_dim(visibilities, block_index * BLOCK_ROW_COUNT, BLOCK_ROW_COUNT, 3)
        first_station_gain = lax.dynamic_slice_in_dim(first_station, block_index * BLOCK_ROW_COUNT, BLOCK_ROW_COUNT, 0)
        second_station_gain = lax.dynamic_slice_in_dim(second_station, block_index * BLOCK_ROW_COUNT, BLOCK_ROW_COUNT, 0)
        return apply_correction(gain_window, block_visibilities, first_station_gain, second_station_gain, filled_row_count[block_index])

    blocks_out = lax.map(one_block, jnp.arange(BLOCKS, dtype=jnp.int32))
    blocks_out = jnp.moveaxis(blocks_out, 0, 3)
    return blocks_out.reshape(FACETS, CHANS, 8, ROWS)
```

```python
import functools

import jax
import jax.numpy as jnp
from jax import lax
from jax.experimental import pallas as pl
from jax.experimental.pallas import tpu as pltpu
from jax.sharding import PartitionSpec as P

ARRAY_STATIONS = 62
GAIN_SLOT_COUNT = 4
MESH = pl.DeviceIdType.MESH
LANES = 128
HALF = 64
COMPS = 8
F32 = jnp.float32
BF16 = jnp.bfloat16


def complex_dot(pairs, conj):
    re = im = None
    for (ar, ai), (br, bi) in pairs:
        if conj:
            pr = ar * br + ai * bi
            pi = ai * br - ar * bi
        else:
            pr = ar * br - ai * bi
            pi = ar * bi + ai * br
        re = pr if re is None else re + pr
        im = pi if im is None else im + pi
    return re, im


def jones(left, data, right):
    a = lambda m, i, j: (m[2 * i + j], m[4 + 2 * i + j])
    mid = {}
    for i in (0, 1):
        for j in (0, 1):
            mid[i, j] = complex_dot(
                [(a(left, i, t), a(data, t, j)) for t in (0, 1)], False
            )
    out = [None] * COMPS
    for i in (0, 1):
        for j in (0, 1):
            re, im = complex_dot(
                [(mid[i, t], a(right, j, t)) for t in (0, 1)], True
            )
            out[2 * i + j], out[4 + 2 * i + j] = re, im
    return out


def pack(gains, send, n, targets):
    slots, st = GAIN_SLOT_COUNT, ARRAY_STATIONS
    chans = gains.shape[1]
    pitch = slots // 2 * COMPS + COMPS // 2
    half = COMPS // 2
    gap8 = jnp.zeros((COMPS, HALF - st), F32)
    gap4 = jnp.zeros((half, HALF - st), F32)

    def slot_of(c, t):
        t = min(t, n * slots - 1)
        return gains[0, c, :, t * st : (t + 1) * st]

    for b in targets:
        for c in range(chans):
            at = (b * chans + c) * pitch
            for pair in range(slots // 2):
                t = b * slots + 2 * pair
                send[at + pair * COMPS : at + (pair + 1) * COMPS, :] = jnp.concatenate(
                    [slot_of(c, t), gap8, slot_of(c, t + 1), gap8], axis=1
                )
            last = slot_of(c, (b + 1) * slots)
            at += slots // 2 * COMPS
            send[at : at + half, :] = jnp.concatenate(
                [last[:half], gap4, last[half:], gap4], axis=1
            )


def kernel(
    n,
    pols,
    gains_hbm,
    vis_hbm,
    first_hbm,
    second_hbm,
    filled_hbm,
    dir_hbm,
    out_ref,
    gains,
    vis,
    stations,
    filled,
    dirs,
    send,
    recv,
    planar,
    stage,
    table,
    in_sem,
    send_sem,
    recv_sem,
    ready,
):
    facets, chans, comps, rows = vis.shape
    slots = GAIN_SLOT_COUNT
    per_slot = rows // slots
    pitch = slots // 2 * COMPS + COMPS // 2
    slab = chans * pitch
    group = COMPS // chans
    bts = n // pols
    my_bt, my_pol = lax.axis_index("bt"), lax.axis_index("pol")
    me = my_bt * pols + my_pol
    everyone = [(b, p) for b in range(bts) for p in range(pols)]

    copies = [
        pltpu.make_async_copy(src, dst, in_sem.at[i])
        for src, dst, i in [
            (gains_hbm, gains, 0),
            (first_hbm, stations.at[0], 1),
            (second_hbm, stations.at[1], 1),
            (dir_hbm, dirs, 2),
            (filled_hbm, filled, 3),
            (vis_hbm, vis, 4),
        ]
    ]
    copies[0].start()
    barrier = pltpu.get_barrier_semaphore()
    for b, p in everyone:
        mate = jnp.logical_and(my_bt == b, my_pol != p)

        @pl.when(jnp.logical_or(my_bt < b, mate))
        def _():
            pl.semaphore_signal(
                barrier, inc=1, device_id={"bt": b, "pol": p}, device_id_type=MESH
            )

    for copy in copies[1:]:
        copy.start()
    pl.semaphore_wait(barrier, my_bt * pols + pols - 1)
    for b, p in everyone:

        @pl.when(my_bt > b)
        def _():
            pl.semaphore_signal(
                ready.at[me], inc=1, device_id={"bt": b, "pol": p}, device_id_type=MESH
            )

    copies[0].wait()

    mine = pl.ds(pl.multiple_of(me * slab, 8), slab)

    def post(b, p):
        t = b * pols + p

        @pl.when(my_bt < b)
        def _():
            pl.semaphore_wait(ready.at[t], 1)

        @pl.when(me != t)
        def _():
            pltpu.make_async_remote_copy(
                src_ref=send.at[pl.ds(t * slab, slab), :],
                dst_ref=recv.at[mine, :],
                send_sem=send_sem,
                recv_sem=recv_sem.at[my_bt],
                device_id={"bt": b, "pol": p},
                device_id_type=MESH,
            ).start()

    pack(gains, send, n, range(pols))
    for p in range(pols):
        post(0, p)
    pack(gains, send, n, range(pols, n))
    pltpu.make_async_copy(send.at[mine, :], recv.at[mine, :], recv_sem.at[my_bt]).start()
    for b, p in everyone[pols:]:
        post(b, p)

    pltpu.make_async_copy(stations, stations, in_sem.at[1]).wait()
    copies[3].wait()
    copies[4].wait()
    copies[5].wait()
    ck = chans * comps
    total = facets * ck
    prow = lax.broadcasted_iota(jnp.int32, (total, total), 0)
    pcol = lax.broadcasted_iota(jnp.int32, (total, total), 1)
    facet_of = pcol // ck
    dir_of = jnp.zeros_like(pcol)
    for f in range(facets):
        dir_of = jnp.where(facet_of == f, dirs[f], dir_of)
    inner = lax.rem(pcol, ck)
    seat = lax.rem(dir_of, group) * chans + inner // comps
    target = (dir_of // group * comps + lax.rem(inner, comps)) * COMPS + seat
    perm = jnp.where(prow == target, 1.0, 0.0).astype(BF16)
    flat = vis[...].astype(F32).reshape(total, rows).astype(BF16)
    planar[...] = jnp.dot(perm, flat, preferred_element_type=F32)

    tile = (COMPS, per_slot)
    col = lax.broadcasted_iota(jnp.int32, tile, 1)
    frac = (col.astype(F32) + 0.5) / per_slot
    live_rows = filled[0]
    in_low = col < HALF

    row = lax.broadcasted_iota(jnp.int32, (LANES, per_slot), 0)
    mcol = lax.broadcasted_iota(jnp.int32, (LANES, per_slot), 1)
    station = lax.rem(row, HALF)
    lower = row < HALF
    mfrac = (mcol.astype(F32) + 0.5) / per_slot
    for s in range(slots):
        now, then = 1.0 - mfrac, mfrac
        weight = jnp.where(lower, now, then) if s % 2 == 0 else jnp.where(lower, then, now)
        live = (mcol + s * per_slot) < live_rows
        lt = jnp.where((station == stations[0, s : s + 1, :]) & live, weight, 0.0)
        rt = jnp.where(station == stations[1, s : s + 1, :], weight, 0.0)
        both = jnp.concatenate([lt, rt], axis=1).astype(BF16)
        table[s, 0:LANES, :] = both
        table[s, LANES : 2 * LANES, :] = both

    for g in range(facets // group):
        for b in range(g * group // pols, -(-(g + 1) * group // pols)):
            part = recv.at[pl.ds(b * pols * slab, pols * slab), :]
            pltpu.make_async_copy(part, part, recv_sem.at[b]).wait()
        base = g * group * slab
        load = lambda at: recv[pl.ds(base + at, COMPS, stride=pitch), :]
        pairs = [[load(p * COMPS + k) for k in range(comps)] for p in range(slots // 2)]
        tails = [load(slots // 2 * COMPS + k) for k in range(comps // 2)]

        def spread(s):
            x = pairs[s // 2]
            if s % 2 == 1:
                if s + 1 < slots:
                    nxt = pairs[(s + 1) // 2]
                else:
                    nxt = [tails[k] if k < comps // 2 else pltpu.roll(tails[k - comps // 2], HALF, 1) for k in range(comps)]
                x = [jnp.where(in_low, b, a) for a, b in zip(x, nxt)]
            x = jnp.concatenate(x, axis=0)
            hi = x.astype(BF16)
            lo = (x - hi.astype(F32)).astype(BF16)
            both = jnp.dot(
                jnp.concatenate([hi, lo], axis=1), table[s], preferred_element_type=F32
            )
            cut = lambda k: slice(k * COMPS, (k + 1) * COMPS)
            return [both[cut(k), 0:per_slot] for k in range(comps)], [both[cut(k), per_slot:] for k in range(comps)]
        for s in range(slots):
            left, right = spread(s)
            data = [
                planar[(g * comps + k) * COMPS : (g * comps + k + 1) * COMPS, s * per_slot : (s + 1) * per_slot]
                for k in range(comps)
            ]
            for k, plane in enumerate(jones(left, data, right)):
                stage[s, pl.ds(g * COMPS * comps + k, COMPS, stride=comps), :] = plane

    by_dir = stage.reshape(slots, facets, ck, per_slot)
    for f in range(facets):
        for c in range(chans):
            for s in range(slots):
                out_ref[f, c, :, s * per_slot : (s + 1) * per_slot] = by_dir[
                    s, dirs[f], c * comps : (c + 1) * comps, :
                ].astype(BF16)

    sent = send.at[pl.ds(0, (n - 1) * slab), :]
    pltpu.make_async_copy(sent, sent, send_sem).wait()


def shards(gains, visibilities, first_station, second_station, filled_row_count, facet_dir):
    n = lax.axis_size(("bt", "pol"))
    pols = lax.axis_size("pol")
    facets, chans, comps, rows = visibilities.shape
    slots = GAIN_SLOT_COUNT
    slab = chans * (slots // 2 * COMPS + COMPS // 2)
    total = facets * chans * comps
    anywhere = pl.BlockSpec(memory_space=pltpu.HBM)
    return pl.pallas_call(
        functools.partial(kernel, n, pols),
        out_shape=pltpu.VMEM(visibilities.shape, BF16),
        in_specs=[anywhere] * 6,
        out_specs=pl.BlockSpec(memory_space=pltpu.VMEM),
        scratch_shapes=[
            pltpu.VMEM(gains.shape, F32),
            pltpu.VMEM(visibilities.shape, BF16),
            pltpu.VMEM((2, slots, rows // slots), jnp.int32),
            pltpu.SMEM(filled_row_count.shape, jnp.int32),
            pltpu.SMEM(facet_dir.shape, jnp.int32),
            pltpu.VMEM((n * slab, LANES), F32),
            pltpu.VMEM((n * slab, LANES), F32),
            pltpu.VMEM((total, rows), F32),
            pltpu.VMEM((slots, total, rows // slots), F32),
            pltpu.VMEM((slots, 2 * LANES, 2 * (rows // slots)), BF16),
            pltpu.SemaphoreType.DMA((5,)),
            pltpu.SemaphoreType.DMA,
            pltpu.SemaphoreType.DMA((n // pols,)),
            pltpu.SemaphoreType.REGULAR((n,)),
        ],
        compiler_params=pltpu.CompilerParams(collective_id=0, has_side_effects=True),
        name="jones",
    )(
        gains,
        visibilities,
        first_station.reshape(slots, rows // slots),
        second_station.reshape(slots, rows // slots),
        filled_row_count,
        facet_dir,
    )


def solution(mesh):
    return jax.shard_map(
        shards,
        mesh=mesh,
        in_specs=(
            P(("obs", "bt", "pol"), "freq", None, None),
            P("obs", "freq", None, ("bt", "pol")),
            P(("obs", "bt", "pol")),
            P(("obs", "bt", "pol")),
            P(("obs", "bt", "pol")),
            P("obs"),
        ),
        out_specs=P("obs", "freq", None, ("bt", "pol")),
        check_vma=False,
    )
```
